256 devices in a mesh: groups: 2 (over z), grid: 16 (over y, core), orb: 8 (over x).
Axes of the slice: x: 8, y: 8, z: 2, core: 2. Of those that a mesh axis runs over, the one named last changes fastest.
The devices are a block of a 8x8x16 slice.
Arguments:
- orbitals: float32 [64, 2, 128, 128, 128], P(('groups', 'orb'), None, 'grid'), parts along dimension 0, may hold values from -6 to 6
- v_local: float32 [256, 128, 128], P(('groups', 'grid')), parts along dimension 0, may hold values from -24 to 24
- occupations: float32 [64], P('groups'), parts along dimension 0, may hold values from 0.05 to 0.5
Outputs:
- orbitals_next: float32 [64, 2, 128, 128, 128], P(('groups', 'orb'), None, 'grid'), parts along dimension 0
The draws below stay inside these ranges and needn't reach their ends.
There are 2 independent parts, one for each index of `groups`. The reference program is written for one: setup_inputs(seed, part) draws one part's arguments, and reference() takes and returns one part's arrays. A program takes and returns all parts, laid end to end along the dimension named above; each array names one. Nothing has to cross between parts.
All inputs are finite; a program needn't handle non-finite values.
Results may differ from the reference program's by a relative error of at most 0.00035.
Values sent between devices are 32-bit elements; how exact they have to be, the bound alone decides.
A program may use at most 64 MiB of HBM per device.

```python
import math
import jax
import jax.numpy as jnp
from jax import lax

NX = 128
NY = 128
NZ = 128
ORB = 32


def block_levels(rng, dims, split, low, high):
    def one(dim, blocks):
        steps = jax.random.uniform(jax.random.fold_in(jax.random.fold_in(rng, 6), dim), (blocks,), jnp.float32, low / len(split), high / len(split))
        return jnp.repeat(jnp.exp(steps), dims[dim] // blocks).reshape((-1,) + (1,) * (len(dims) - dim - 1))

    factor_of = one(*split[0])
    for cut in split[1:]:
        factor_of = factor_of * one(*cut)
    return factor_of


def bell_draw(rng, shape, spread, reach, pieces=(), dtype=jnp.bfloat16):
    array = jax.random.normal(rng, shape, jnp.float32) * spread
    if len(pieces) > 0:
        array = block_levels(rng, shape, pieces, -0.22, 0.18) * array
    return jnp.clip(array, min=-reach, max=reach).astype(dtype)


def setup_inputs(seed: int = 0, part: int = 0) -> dict:
    splits = jax.random.split(jax.random.key(seed), 4)
    own_keys = jax.random.split(jax.random.fold_in(splits[3], part), 4)
    return {
        "orbitals": bell_draw(own_keys[0], (ORB, 2, NX, NY, NZ), 1.0, 6.0, ((0, 8), (2, 16)), jnp.float32),
        "v_local": bell_draw(own_keys[1], (NX, NY, NZ), 4.0, 24.0, ((0, 16),), jnp.float32),
        "occupations": jnp.clip(jnp.exp(jax.random.uniform(own_keys[2], (ORB,), jnp.float32, math.log(0.05), math.log(0.5))), 0.05, 0.5),
    }


TIME_STEP = 0.05
KINETIC_RATE = 0.1
HARTREE_SCALE = math.pi


def wave_squared(length):
    wavenumber = jnp.fft.fftfreq(length).astype(jnp.float32) * (2.0 * math.pi)
    return wavenumber * wavenumber


def reference(orbitals, v_local, occupations):
    waves = wave_squared(NX)[:, None, None] + wave_squared(NY)[None, :, None] + wave_squared(NZ)[None, None, :]
    kinetic_turn = -KINETIC_RATE * waves
    propagator = lax.complex(jnp.cos(kinetic_turn), jnp.sin(kinetic_turn))
    spectrum = jnp.fft.fftn(lax.complex(orbitals[:, 0], orbitals[:, 1]), axes=(1, 2, 3))
    evolved = jnp.fft.ifftn(spectrum * propagator[None], axes=(1, 2, 3))
    evolved_re = jnp.real(evolved)
    evolved_im = jnp.imag(evolved)
    density = jnp.sum(occupations[:, None, None, None] * (evolved_re * evolved_re + evolved_im * evolved_im), axis=0)
    anchor = waves <= 0.0
    kernel = jnp.where(anchor, 0.0, HARTREE_SCALE / jnp.where(anchor, 1.0, waves))
    hartree = jnp.real(jnp.fft.ifftn(jnp.fft.fftn(density) * kernel))
    phase_angle = TIME_STEP * (v_local + hartree)
    cosine = jnp.cos(phase_angle)[None]
    sine = jnp.sin(phase_angle)[None]
    out_re = evolved_re * cosine + evolved_im * sine
    out_im = evolved_im * cosine - evolved_re * sine
    return jnp.stack([out_re, out_im], 1).astype(jnp.float32)
```

```python
import functools
import math

import jax
import jax.numpy as jnp
import numpy as np
from jax import lax
from jax.experimental import pallas as pl
from jax.experimental.pallas import tpu as pltpu
from jax.sharding import PartitionSpec as P

TIME_STEP = 0.05
KINETIC_RATE = 0.1
HARTREE_SCALE = math.pi
HIGHEST = lax.Precision.HIGHEST
MESH = pl.DeviceIdType.MESH


def wave_squared(length):
    mode_ids = np.arange(length)
    signed = np.where(mode_ids < (length + 1) // 2, mode_ids, mode_ids - length)
    return (2.0 * math.pi * signed / length) ** 2


def kinetic_table(length):
    phase = np.exp(-1j * KINETIC_RATE * wave_squared(length))
    circulant = np.fft.ifft(phase)
    ids = np.arange(length)
    full = circulant[(ids[:, None] - ids[None, :]) % length]
    return np.block([[full.real, -full.imag], [full.imag, full.real]]).astype(np.float32)


def hartley_table(length):
    ids = np.arange(length)
    angle = 2.0 * math.pi * (ids[:, None] * ids[None, :] % length) / length
    return ((np.cos(angle) + np.sin(angle)) / math.sqrt(length)).astype(np.float32)


def dot(left, right):
    return jnp.dot(left, right, precision=HIGHEST, preferred_element_type=jnp.float32)


def swap(block):
    return jnp.transpose(block, (1, 0, 2))


def kernel(
    grid_count,
    orb_count,
    occ_ref,
    psi_ref,
    left_x,
    left_y,
    right_z,
    hart_x,
    hart_y,
    hart_z,
    sq_y,
    sq_z,
    evolved_ref,
    hartree_ref,
    own,
    lines_y,
    send_a,
    recv_a,
    lines_x,
    send_b,
    density,
    parts,
    modes,
    modes_in,
    tiles,
    pencil,
    pencil_out,
    tiles_in,
    tiles_out,
    plane_in,
    plane,
    slabs,
    load_sem,
    recv_sem,
    recv_b_sem,
    send_sem,
    hart_send,
    hart_recv,
):
    g = lax.axis_index("grid")
    o = lax.axis_index("orb")
    layers, _, planes, count_y, count_z = own.shape
    count_x = planes * grid_count
    block_y = count_y // grid_count
    block_k = count_x // orb_count

    def load(l):
        return pltpu.make_async_copy(psi_ref.at[l], own.at[l], load_sem.at[l])

    for l in range(layers):
        load(l).start()

    barrier = pltpu.get_barrier_semaphore()

    def greet(axis, me, count):
        def one(off, carry):
            pl.semaphore_signal(
                barrier, inc=1, device_id={axis: lax.rem(me + off, count)}, device_id_type=MESH
            )
            return carry

        lax.fori_loop(1, count, one, 0)

    greet("grid", g, grid_count)
    greet("orb", o, orb_count)

    def send_all(axis, me, count, src, dst, s_sem, r_sem):
        def one(off, carry):
            to = lax.rem(me + off, count)
            pltpu.make_async_remote_copy(
                src_ref=src(to),
                dst_ref=dst,
                send_sem=s_sem,
                recv_sem=r_sem,
                device_id={axis: to},
                device_id_type=MESH,
            ).start()
            return carry

        lax.fori_loop(1, count, one, 0)

    def wait_for(ref, sem):
        pltpu.make_async_copy(ref, ref, sem).wait()

    def rows(start, size):
        return pl.ds(pl.multiple_of(start, 8), size)

    def along_y(l):
        load(l).wait()

        def pair(i, carry):
            both = [
                jnp.concatenate([own[l, 0, 2 * i + k], own[l, 1, 2 * i + k]], axis=0) for k in (0, 1)
            ]
            out = dot(left_y[...], jnp.concatenate(both, axis=1))
            lines_y[2 * i] = out[:, :count_z]
            lines_y[2 * i + 1] = out[:, count_z:]
            return carry

        lax.fori_loop(0, planes // 2, pair, 0)

    quads = 4 if grid_count % 4 == 0 else 1
    chunk_y = count_y // quads

    def along_z(l):
        def quad(i, carry):
            start = lax.rem(g // (grid_count // quads) + i, quads) * chunk_y
            sides = []
            for c in (0, 1):
                block = lines_y[:, rows(c * count_y + start, chunk_y), :]
                sides.append(swap(block).reshape(chunk_y * planes, count_z))
            out = dot(jnp.concatenate(sides, axis=1), right_z[...])
            for c in (0, 1):
                part = out[:, c * count_z : (c + 1) * count_z]
                send_a[l, pl.ds(start, chunk_y), c] = part.reshape(chunk_y, planes, count_z)
            return carry

        lax.fori_loop(0, quads, quad, 0)

    def forward(l):
        along_y(l)
        along_z(l)

    def launch_forward(l):
        def src(to):
            return send_a.at[l, pl.ds(to * block_y, block_y)]

        dst = recv_a.at[l, :, :, rows(g * planes, planes), :]
        pltpu.make_async_copy(src(g), dst, recv_sem.at[l]).start()
        send_all("grid", g, grid_count, src, dst, send_sem.at[0], recv_sem.at[l])

    def across_x(l):
        wait_for(recv_a.at[l], recv_sem.at[l])
        weight = occ_ref[o * layers + l]

        def pair(i, carry):
            both = [recv_a[l, 2 * i + k].reshape(2 * count_x, count_z) for k in (0, 1)]
            out = dot(left_x[...], jnp.concatenate(both, axis=1))
            for k in (0, 1):
                part = out[:, k * count_z : (k + 1) * count_z]
                lines_x[2 * i + k] = part
                squares = part[:count_x] * part[:count_x] + part[count_x:] * part[count_x:]
                if l == 0:
                    density[2 * i + k] = weight * squares
                else:
                    density[2 * i + k] += weight * squares
            return carry

        lax.fori_loop(0, block_y // 2, pair, 0)

        def turn(i, carry):
            for c in (0, 1):
                block = lines_x[:, rows(c * count_x + i * planes, planes), :]
                send_b[l, c, rows(i * planes, planes)] = swap(block)
            return carry

        lax.fori_loop(0, grid_count, turn, 0)

    def launch_back(l):
        def src(to):
            return send_b.at[l, :, pl.ds(to * planes, planes)]

        dst = evolved_ref.at[l, :, :, rows(g * block_y, block_y), :]
        pltpu.make_async_copy(src(g), dst, recv_b_sem).start()
        send_all("grid", g, grid_count, src, dst, send_sem.at[1], recv_b_sem)

    forward(0)
    pl.semaphore_wait(barrier, grid_count - 1 + orb_count - 1)
    launch_forward(0)
    for l in range(1, layers):
        forward(l)
        launch_forward(l)
    across_x(0)
    launch_back(0)
    for l in range(1, layers):
        across_x(l)

    send_all("orb", o, orb_count, lambda to: density.at[to], parts.at[o], hart_send.at[0], hart_recv.at[0])
    parts[o] = jnp.zeros((count_x, count_z), jnp.float32)
    wait_for(parts.at[pl.ds(0, orb_count - 1)], hart_recv.at[0])
    total = density[o]
    for k in range(orb_count):
        total += parts[k]
    modes[...] = dot(dot(hart_x[...], total), hart_z[...])

    send_all(
        "orb", o, orb_count, lambda to: modes.at[rows(to * block_k, block_k)], modes_in.at[o], hart_send.at[1], hart_recv.at[1]
    )
    modes_in[o] = modes[rows(o * block_k, block_k)]
    wait_for(modes_in.at[pl.ds(0, orb_count - 1)], hart_recv.at[1])
    tiles[...] = swap(modes_in[...])

    send_all(
        "grid", g, grid_count, lambda to: tiles.at[to], pencil.at[rows(g * block_y, block_y)], hart_send.at[2], hart_recv.at[2]
    )
    pencil[rows(g * block_y, block_y)] = tiles[g]
    if layers > 1:
        launch_back(1)
    wait_for(pencil.at[pl.ds(0, count_y - block_y)], hart_recv.at[2])

    mode_x = o * block_k + g
    signed_x = jnp.where(mode_x < (count_x + 1) // 2, mode_x, mode_x - count_x).astype(jnp.float32)
    wave_x = signed_x * (2.0 * math.pi / count_x)
    waves = wave_x * wave_x + sq_y[...] + sq_z[...]
    anchor = waves <= 0.0
    scale = jnp.where(anchor, 0.0, HARTREE_SCALE / jnp.where(anchor, 1.0, waves))
    pencil_out[...] = dot(hart_y[...], dot(hart_y[...], pencil[...]) * scale)

    send_all(
        "grid", g, grid_count, lambda to: pencil_out.at[rows(to * block_y, block_y)], tiles_in.at[g], hart_send.at[3], hart_recv.at[3]
    )
    tiles_in[g] = pencil_out[rows(g * block_y, block_y)]
    if layers > 2:
        launch_back(2)
    wait_for(tiles_in.at[pl.ds(0, grid_count - 1)], hart_recv.at[3])
    tiles_out[...] = swap(tiles_in[...])

    send_all(
        "orb", o, orb_count, lambda to: tiles_out.at[to], plane_in.at[rows(o * block_k, block_k)], hart_send.at[4], hart_recv.at[4]
    )
    plane_in[rows(o * block_k, block_k)] = tiles_out[o]
    wait_for(plane_in.at[pl.ds(0, count_x - block_k)], hart_recv.at[4])
    plane[...] = dot(dot(hart_x[...], plane_in[...]), hart_z[...])

    mine = slabs.at[o]
    send_all(
        "grid", g, grid_count, lambda to: plane.at[rows(to * planes, planes)], slabs.at[o, g], hart_send.at[5], hart_recv.at[5]
    )
    slabs[o, g] = plane[rows(g * planes, planes)]
    for l in range(3, layers):
        launch_back(l)
    wait_for(mine.at[pl.ds(0, grid_count - 1)], hart_recv.at[5])

    send_all("orb", o, orb_count, lambda to: slabs.at[o], slabs.at[o], hart_send.at[6], hart_recv.at[6])
    wait_for(slabs.at[pl.ds(0, orb_count - 1)], hart_recv.at[6])

    def spread(i, carry):
        hartree_ref[:, rows(i * block_y, block_y), :] = swap(slabs[:, i])
        return carry

    lax.fori_loop(0, grid_count, spread, 0)

    wait_for(evolved_ref, recv_b_sem)
    sent_a = send_a.at[:, pl.ds(0, count_y - block_y)]
    wait_for(sent_a, send_sem.at[0])
    sent_b = send_b.at[:, :, pl.ds(0, count_x - planes)]
    wait_for(sent_b, send_sem.at[1])
    wait_for(density.at[pl.ds(0, orb_count - 1)], hart_send.at[0])
    wait_for(modes.at[pl.ds(0, count_x - block_k)], hart_send.at[1])
    wait_for(tiles.at[pl.ds(0, grid_count - 1)], hart_send.at[2])
    wait_for(pencil_out.at[pl.ds(0, count_y - block_y)], hart_send.at[3])
    wait_for(tiles_out.at[pl.ds(0, orb_count - 1)], hart_send.at[4])
    wait_for(plane.at[pl.ds(0, count_x - planes)], hart_send.at[5])
    wait_for(slabs.at[pl.ds(0, orb_count - 1)], hart_send.at[6])


def body(grid_count, orb_count, orbitals, v_local, occupations):
    layers, _, planes, count_y, count_z = orbitals.shape
    count_x = planes * grid_count
    block_y = count_y // grid_count
    block_k = count_x // orb_count
    assert block_y == orb_count and block_k == grid_count

    f32 = jnp.float32
    tables = (
        kinetic_table(count_x),
        kinetic_table(count_y),
        kinetic_table(count_z).T,
        hartley_table(count_x),
        hartley_table(count_y),
        hartley_table(count_z),
        wave_squared(count_y).astype(np.float32)[:, None],
        wave_squared(count_z).astype(np.float32)[None, :],
    )
    shared = {}
    tables = [shared.setdefault((t.shape, t.tobytes()), jnp.asarray(t)) for t in tables]
    vmem = pl.BlockSpec(memory_space=pltpu.VMEM)
    anyspace = pl.BlockSpec(memory_space=pl.ANY)
    evolved, hartree = pl.pallas_call(
        functools.partial(kernel, grid_count, orb_count),
        out_shape=(
            jax.ShapeDtypeStruct(orbitals.shape, f32),
            jax.ShapeDtypeStruct((planes, count_y, count_z), f32),
        ),
        in_specs=[pl.BlockSpec(memory_space=pltpu.SMEM), anyspace] + [vmem] * 8,
        out_specs=(anyspace, vmem),
        scratch_shapes=[
            pltpu.VMEM(orbitals.shape, f32),
            pltpu.VMEM((planes, 2 * count_y, count_z), f32),
            pltpu.VMEM((layers, count_y, 2, planes, count_z), f32),
            pltpu.VMEM((layers, block_y, 2, count_x, count_z), f32),
            pltpu.VMEM((block_y, 2 * count_x, count_z), f32),
            pltpu.VMEM((layers, 2, count_x, block_y, count_z), f32),
            pltpu.VMEM((block_y, count_x, count_z), f32),
            pltpu.VMEM((orb_count, count_x, count_z), f32),
            pltpu.VMEM((count_x, count_z), f32),
            pltpu.VMEM((orb_count, block_k, count_z), f32),
            pltpu.VMEM((grid_count, block_y, count_z), f32),
            pltpu.VMEM((count_y, count_z), f32),
            pltpu.VMEM((count_y, count_z), f32),
            pltpu.VMEM((grid_count, block_y, count_z), f32),
            pltpu.VMEM((block_y, grid_count, count_z), f32),
            pltpu.VMEM((count_x, count_z), f32),
            pltpu.VMEM((count_x, count_z), f32),
            pltpu.VMEM((orb_count, grid_count, planes, count_z), f32),
            pltpu.SemaphoreType.DMA((layers,)),
            pltpu.SemaphoreType.DMA((layers,)),
            pltpu.SemaphoreType.DMA,
            pltpu.SemaphoreType.DMA((2,)),
            pltpu.SemaphoreType.DMA((7,)),
            pltpu.SemaphoreType.DMA((7,)),
        ],
        compiler_params=pltpu.CompilerParams(
            collective_id=0, has_side_effects=True, vmem_limit_bytes=48 * 1024 * 1024
        ),
        name="step",
    )(occupations, orbitals, *tables)

    theta = TIME_STEP * (v_local + hartree)
    cosine = jnp.cos(theta)
    sine = jnp.sin(theta)
    real_part, imag_part = evolved[:, 0], evolved[:, 1]
    return jnp.stack(
        [real_part * cosine + imag_part * sine, imag_part * cosine - real_part * sine], 1
    )


def solution(mesh):
    return jax.shard_map(
        functools.partial(body, mesh.shape["grid"], mesh.shape["orb"]),
        mesh=mesh,
        in_specs=(
            P(("groups", "orb"), None, "grid", None, None),
            P(("groups", "grid"), None, None),
            P("groups"),
        ),
        out_specs=P(("groups", "orb"), None, "grid", None, None),
        check_vma=False,
    )
```

```python
import functools
import math

import jax
import jax.numpy as jnp
import numpy as np
from jax import lax
from jax.experimental import pallas as pl
from jax.experimental.pallas import tpu as pltpu
from jax.sharding import PartitionSpec as P

TIME_STEP = 0.05
KINETIC_RATE = 0.1
HARTREE_SCALE = math.pi
HIGHEST = lax.Precision.HIGHEST
MESH = pl.DeviceIdType.MESH


def wave_squared(length):
    mode_ids = np.arange(length)
    signed = np.where(mode_ids < (length + 1) // 2, mode_ids, mode_ids - length)
    return (2.0 * math.pi * signed / length) ** 2


def kinetic_table(length):
    phase = np.exp(-1j * KINETIC_RATE * wave_squared(length))
    circulant = np.fft.ifft(phase)
    ids = np.arange(length)
    full = circulant[(ids[:, None] - ids[None, :]) % length]
    return np.block([[full.real, -full.imag], [full.imag, full.real]]).astype(np.float32)


def hartley_table(length):
    ids = np.arange(length)
    angle = 2.0 * math.pi * (ids[:, None] * ids[None, :] % length) / length
    return ((np.cos(angle) + np.sin(angle)) / math.sqrt(length)).astype(np.float32)


def dot(left, right):
    return jnp.dot(left, right, precision=HIGHEST, preferred_element_type=jnp.float32)


def swap(block):
    return jnp.transpose(block, (1, 0, 2))


def kernel(
    grid_count,
    orb_count,
    table_slots,
    occ_hbm,
    psi_ref,
    v_hbm,
    *refs,
):
    n_tables = len(set(table_slots))
    tables_hbm = refs[:n_tables]
    out_ref = refs[n_tables]
    tables = refs[n_tables + 1 : 2 * n_tables + 1]
    (
    occ_ref,
    v_ref,
    own,
    lines_y,
    send_a,
    recv_a,
    lines_x,
    send_b,
    density,
    spectrum,
    parts,
    tiles,
    pencil,
    pencil_out,
    tiles_in,
    tiles_out,
    plane_in,
    plane,
    slabs,
    arrived,
    cosine,
    sine,
    table_sem,
    load_sem,
    recv_sem,
    recv_b_sem,
    send_sem,
    hart_send,
    hart_recv,
    ) = refs[2 * n_tables + 1 :]
    left_x, left_y, right_z, hart_x, hart_y, hart_z = [tables[i] for i in table_slots]
    g = lax.axis_index("grid")
    o = lax.axis_index("orb")
    layers, _, planes, count_y, count_z = own.shape
    count_x = planes * grid_count
    block_y = count_y // grid_count
    block_k = count_x // orb_count

    def load(l):
        return pltpu.make_async_copy(psi_ref.at[l], own.at[l], load_sem.at[l])

    def fetch(i):
        return pltpu.make_async_copy(tables_hbm[i], tables[i], table_sem.at[i])

    occ_copy = pltpu.make_async_copy(occ_hbm, occ_ref, table_sem.at[n_tables])
    v_copy = pltpu.make_async_copy(v_hbm, v_ref, table_sem.at[n_tables + 1])
    load(0).start()
    for i in range(n_tables):
        fetch(i).start()
    for l in range(1, layers):
        load(l).start()
    occ_copy.start()
    v_copy.start()

    barrier = pltpu.get_barrier_semaphore()

    def greet(axis, me, count):
        def one(off, carry):
            pl.semaphore_signal(
                barrier, inc=1, device_id={axis: lax.rem(me + off, count)}, device_id_type=MESH
            )
            return carry

        lax.fori_loop(1, count, one, 0)

    greet("grid", g, grid_count)
    greet("orb", o, orb_count)

    def send_all(axis, me, count, src, dst, s_sem, r_sem):
        def one(off, carry):
            to = lax.rem(me + off, count)
            pltpu.make_async_remote_copy(
                src_ref=src(to),
                dst_ref=dst,
                send_sem=s_sem,
                recv_sem=r_sem,
                device_id={axis: to},
                device_id_type=MESH,
            ).start()
            return carry

        lax.fori_loop(1, count, one, 0)

    def wait_for(ref, sem):
        pltpu.make_async_copy(ref, ref, sem).wait()

    def rows(start, size):
        return pl.ds(pl.multiple_of(start, 8), size)

    def along_y(l):
        load(l).wait()

        def pair(i, carry):
            both = [
                jnp.concatenate([own[l, 0, 2 * i + k], own[l, 1, 2 * i + k]], axis=0) for k in (0, 1)
            ]
            out = dot(left_y[...], jnp.concatenate(both, axis=1))
            lines_y[2 * i] = out[:, :count_z]
            lines_y[2 * i + 1] = out[:, count_z:]
            return carry

        lax.fori_loop(0, planes // 2, pair, 0)

    quads = 4 if grid_count % 4 == 0 else 1
    chunk_y = count_y // quads
    targets = grid_count // quads

    def along_z(l):
        def quad(i, carry):
            first = lax.rem(g // targets + i, quads) * targets
            start = first * block_y
            sides = []
            for c in (0, 1):
                block = lines_y[:, rows(c * count_y + start, chunk_y), :]
                sides.append(swap(block).reshape(chunk_y * planes, count_z))
            out = dot(jnp.concatenate(sides, axis=1), right_z[...])
            for c in (0, 1):
                part = out[:, c * count_z : (c + 1) * count_z]
                send_a[l, pl.ds(start, chunk_y), c] = part.reshape(chunk_y, planes, count_z)
            if l == 0:

                @pl.when(i == 0)
                def _():
                    pl.semaphore_wait(barrier, grid_count - 1 + orb_count - 1)

            return carry

        lax.fori_loop(0, quads, quad, 0)

    def forward(l):
        along_y(l)
        along_z(l)
        launch_forward(l)

    def launch_forward(l):
        def src(to):
            return send_a.at[l, pl.ds(to * block_y, block_y)]

        dst = recv_a.at[l, :, :, rows(g * planes, planes), :]
        pltpu.make_async_copy(src(g), dst, recv_sem.at[l]).start()
        send_all("grid", g, grid_count, src, dst, send_sem.at[0], recv_sem.at[l])

    def sum_modes(y):
        two = dot(hart_x[...], jnp.concatenate([density[y], density[y + 1]], axis=1))
        two = dot(jnp.concatenate([two[:, :count_z], two[:, count_z:]], axis=0), hart_z[...])
        spectrum[y] = two[:count_x]
        spectrum[y + 1] = two[count_x:]
        pair = pl.ds(y, 2)
        send_all(
            "orb",
            o,
            orb_count,
            lambda to: spectrum.at[pair, rows(to * block_k, block_k), :],
            parts.at[o, pair],
            hart_send.at[0],
            hart_recv.at[0],
        )

    def across_x(l):
        wait_for(recv_a.at[l], recv_sem.at[l])
        weight = occ_ref[o * layers + l]

        def pair(i, carry):
            both = [recv_a[l, 2 * i + k].reshape(2 * count_x, count_z) for k in (0, 1)]
            out = dot(left_x[...], jnp.concatenate(both, axis=1))
            for k in (0, 1):
                part = out[:, k * count_z : (k + 1) * count_z]
                lines_x[2 * i + k] = part
                squares = part[:count_x] * part[:count_x] + part[count_x:] * part[count_x:]
                if l == 0:
                    density[2 * i + k] = weight * squares
                else:
                    density[2 * i + k] += weight * squares
            if l == layers - 1:
                sum_modes(2 * i)
            return carry

        lax.fori_loop(0, block_y // 2, pair, 0)

        def turn(i, carry):
            for c in (0, 1):
                block = lines_x[:, rows(c * count_x + i * planes, planes), :]
                send_b[l, c, rows(i * planes, planes)] = swap(block)
            return carry

        lax.fori_loop(0, grid_count, turn, 0)

    def launch_back(l, c=None):
        part = (slice(None),) if c is None else (c,)

        def src(to):
            return send_b.at[(l, *part, pl.ds(to * planes, planes))]

        dst = arrived.at[(l, *part, slice(None), rows(g * block_y, block_y), slice(None))]
        pltpu.make_async_copy(src(g), dst, recv_b_sem.at[l]).start()
        send_all("grid", g, grid_count, src, dst, send_sem.at[1], recv_b_sem.at[l])

    for i in range(n_tables):
        fetch(i).wait()
    for l in range(layers):
        forward(l)
    occ_copy.wait()
    across_x(0)
    launch_back(0)
    for l in range(1, layers):
        across_x(l)

    wait_for(parts.at[pl.ds(0, orb_count - 1)], hart_recv.at[0])
    own_modes = rows(o * block_k, block_k)
    total = spectrum[:, own_modes, :]
    for off in range(1, orb_count):
        total += parts[lax.rem(o + off, orb_count)]
    tiles[...] = swap(total)

    send_all(
        "grid", g, grid_count, lambda to: tiles.at[to], pencil.at[rows(g * block_y, block_y)], hart_send.at[1], hart_recv.at[1]
    )
    pencil[rows(g * block_y, block_y)] = tiles[g]
    launch_back(1, 0)
    wait_for(pencil.at[pl.ds(0, count_y - block_y)], hart_recv.at[1])

    mode_x = o * block_k + g

    def square(mode, count):
        signed = jnp.where(mode < (count + 1) // 2, mode, mode - count).astype(jnp.float32)
        wave = signed * (2.0 * math.pi / count)
        return wave * wave

    mode_y = lax.broadcasted_iota(jnp.int32, (count_y, count_z), 0)
    mode_z = lax.broadcasted_iota(jnp.int32, (count_y, count_z), 1)
    waves = square(mode_x, count_x) + square(mode_y, count_y) + square(mode_z, count_z)
    anchor = waves <= 0.0
    scale = jnp.where(anchor, 0.0, HARTREE_SCALE / jnp.where(anchor, 1.0, waves))
    pencil_out[...] = dot(hart_y[...], dot(hart_y[...], pencil[...]) * scale)

    send_all(
        "grid", g, grid_count, lambda to: pencil_out.at[rows(to * block_y, block_y)], tiles_in.at[g], hart_send.at[2], hart_recv.at[2]
    )
    tiles_in[g] = pencil_out[rows(g * block_y, block_y)]
    launch_back(1, 1)
    launch_back(2)
    wait_for(tiles_in.at[pl.ds(0, grid_count - 1)], hart_recv.at[2])
    tiles_out[...] = swap(tiles_in[...])

    send_all(
        "orb", o, orb_count, lambda to: tiles_out.at[to], plane_in.at[rows(o * block_k, block_k)], hart_send.at[3], hart_recv.at[3]
    )
    plane_in[rows(o * block_k, block_k)] = tiles_out[o]
    wait_for(plane_in.at[pl.ds(0, count_x - block_k)], hart_recv.at[3])
    plane[...] = dot(dot(hart_x[...], plane_in[...]), hart_z[...])

    mine = slabs.at[o]
    send_all(
        "grid", g, grid_count, lambda to: plane.at[rows(to * planes, planes)], slabs.at[o, g], hart_send.at[4], hart_recv.at[4]
    )
    slabs[o, g] = plane[rows(g * planes, planes)]
    launch_back(3)
    wait_for(mine.at[pl.ds(0, grid_count - 1)], hart_recv.at[4])

    send_all("orb", o, orb_count, lambda to: slabs.at[o], slabs.at[o], hart_send.at[5], hart_recv.at[5])
    wait_for(slabs.at[pl.ds(0, orb_count - 1)], hart_recv.at[5])

    v_copy.wait()

    def spread(i, carry):
        part = rows(i * block_y, block_y)
        theta = TIME_STEP * (v_ref[:, part, :] + swap(slabs[:, i]))
        cosine[:, part, :] = jnp.cos(theta)
        sine[:, part, :] = jnp.sin(theta)
        return carry

    lax.fori_loop(0, grid_count, spread, 0)

    for l in range(layers):
        wait_for(arrived.at[l], recv_b_sem.at[l])

        def turn_phase(x, carry):
            real_part, imag_part = arrived[l, 0, x], arrived[l, 1, x]
            out_ref[l, 0, x] = real_part * cosine[x] + imag_part * sine[x]
            out_ref[l, 1, x] = imag_part * cosine[x] - real_part * sine[x]
            return carry

        lax.fori_loop(0, planes, turn_phase, 0)

    sent_a = send_a.at[:, pl.ds(0, count_y - block_y)]
    wait_for(sent_a, send_sem.at[0])
    sent_b = send_b.at[:, :, pl.ds(0, count_x - planes)]
    wait_for(sent_b, send_sem.at[1])
    wait_for(parts.at[pl.ds(0, orb_count - 1)], hart_send.at[0])
    wait_for(tiles.at[pl.ds(0, grid_count - 1)], hart_send.at[1])
    wait_for(pencil_out.at[pl.ds(0, count_y - block_y)], hart_send.at[2])
    wait_for(tiles_out.at[pl.ds(0, orb_count - 1)], hart_send.at[3])
    wait_for(plane.at[pl.ds(0, count_x - planes)], hart_send.at[4])
    wait_for(slabs.at[pl.ds(0, orb_count - 1)], hart_send.at[5])


def body(grid_count, orb_count, orbitals, v_local, occupations):
    layers, _, planes, count_y, count_z = orbitals.shape
    count_x = planes * grid_count
    block_y = count_y // grid_count
    block_k = count_x // orb_count
    assert block_y == orb_count and block_k == grid_count

    f32 = jnp.float32
    tables = (
        kinetic_table(count_x),
        kinetic_table(count_y),
        kinetic_table(count_z).T,
        hartley_table(count_x),
        hartley_table(count_y),
        hartley_table(count_z),
    )
    keys = [(t.shape, t.tobytes()) for t in tables]
    distinct = list(dict.fromkeys(keys))
    slots = tuple(distinct.index(key) for key in keys)
    tables = [jnp.asarray(tables[keys.index(key)]) for key in distinct]
    anyspace = pl.BlockSpec(memory_space=pltpu.HBM)
    return pl.pallas_call(
        functools.partial(kernel, grid_count, orb_count, slots),
        out_shape=pltpu.VMEM(orbitals.shape, f32),
        in_specs=[anyspace] * (3 + len(tables)),
        out_specs=pl.BlockSpec(memory_space=pltpu.VMEM),
        scratch_shapes=[pltpu.VMEM(t.shape, f32) for t in tables]
        + [
            pltpu.SMEM(occupations.shape, f32),
            pltpu.VMEM(v_local.shape, f32),
            pltpu.VMEM(orbitals.shape, f32),
            pltpu.VMEM((planes, 2 * count_y, count_z), f32),
            pltpu.VMEM((layers, count_y, 2, planes, count_z), f32),
            pltpu.VMEM((layers, block_y, 2, count_x, count_z), f32),
            pltpu.VMEM((block_y, 2 * count_x, count_z), f32),
            pltpu.VMEM((layers, 2, count_x, block_y, count_z), f32),
            pltpu.VMEM((block_y, count_x, count_z), f32),
            pltpu.VMEM((block_y, count_x, count_z), f32),
            pltpu.VMEM((orb_count, block_y, block_k, count_z), f32),
            pltpu.VMEM((grid_count, block_y, count_z), f32),
            pltpu.VMEM((count_y, count_z), f32),
            pltpu.VMEM((count_y, count_z), f32),
            pltpu.VMEM((grid_count, block_y, count_z), f32),
            pltpu.VMEM((block_y, grid_count, count_z), f32),
            pltpu.VMEM((count_x, count_z), f32),
            pltpu.VMEM((count_x, count_z), f32),
            pltpu.VMEM((orb_count, grid_count, planes, count_z), f32),
            pltpu.VMEM(orbitals.shape, f32),
            pltpu.VMEM(v_local.shape, f32),
            pltpu.VMEM(v_local.shape, f32),
            pltpu.SemaphoreType.DMA((len(tables) + 2,)),
            pltpu.SemaphoreType.DMA((layers,)),
            pltpu.SemaphoreType.DMA((layers,)),
            pltpu.SemaphoreType.DMA((layers,)),
            pltpu.SemaphoreType.DMA((2,)),
            pltpu.SemaphoreType.DMA((6,)),
            pltpu.SemaphoreType.DMA((6,)),
        ],
        compiler_params=pltpu.CompilerParams(
            collective_id=0, has_side_effects=True, vmem_limit_bytes=48 * 1024 * 1024
        ),
        name="step",
    )(*[pltpu.with_memory_space_constraint(a, pltpu.HBM) for a in (occupations, orbitals, v_local, *tables)])


def solution(mesh):
    return jax.shard_map(
        functools.partial(body, mesh.shape["grid"], mesh.shape["orb"]),
        mesh=mesh,
        in_specs=(
            P(("groups", "orb"), None, "grid", None, None),
            P(("groups", "grid"), None, None),
            P("groups"),
        ),
        out_specs=P(("groups", "orb"), None, "grid", None, None),
        check_vma=False,
    )
```

```python
import functools
import math

import jax
import jax.numpy as jnp
import numpy as np
from jax import lax
from jax.experimental import pallas as pl
from jax.experimental.pallas import tpu as pltpu
from jax.sharding import PartitionSpec as P

TIME_STEP = 0.05
KINETIC_RATE = 0.1
HARTREE_SCALE = math.pi
HIGHEST = lax.Precision.HIGHEST
MESH = pl.DeviceIdType.MESH


def wave_squared(length):
    mode_ids = np.arange(length)
    signed = np.where(mode_ids < (length + 1) // 2, mode_ids, mode_ids - length)
    return (2.0 * math.pi * signed / length) ** 2


def kinetic_table(length):
    phase = np.exp(-1j * KINETIC_RATE * wave_squared(length))
    circulant = np.fft.ifft(phase)
    ids = np.arange(length)
    full = circulant[(ids[:, None] - ids[None, :]) % length]
    return np.block([[full.real, -full.imag], [full.imag, full.real]]).astype(np.float32)


def hartley_table(length):
    ids = np.arange(length)
    angle = 2.0 * math.pi * (ids[:, None] * ids[None, :] % length) / length
    return ((np.cos(angle) + np.sin(angle)) / math.sqrt(length)).astype(np.float32)


def dot(left, right):
    return jnp.dot(left, right, precision=HIGHEST, preferred_element_type=jnp.float32)


def split(value):
    high = value.astype(jnp.bfloat16)
    return high, (value - high.astype(jnp.float32)).astype(jnp.bfloat16)


def dot_table_left(table, value):
    high, low = split(value)
    stacked = jnp.concatenate([high, high, low], axis=0)
    return jnp.dot(table, stacked, preferred_element_type=jnp.float32)


def dot_table_right(value, table):
    high, low = split(value)
    stacked = jnp.concatenate([high, high, low], axis=1)
    return jnp.dot(stacked, table, preferred_element_type=jnp.float32)


def three_parts(table, axis):
    high = table.astype(jnp.bfloat16)
    low = (table - high.astype(np.float32)).astype(jnp.bfloat16)
    return np.concatenate([high, low, high], axis=axis)


def swap(block):
    return jnp.transpose(block, (1, 0, 2))


def kernel(
    grid_count,
    orb_count,
    table_slots,
    occ_hbm,
    psi_ref,
    v_hbm,
    *refs,
):
    n_tables = len(set(table_slots))
    tables_hbm = refs[:n_tables]
    out_ref = refs[n_tables]
    tables = refs[n_tables + 1 : 2 * n_tables + 1]
    (
    occ_ref,
    v_ref,
    own,
    lines_y,
    send_a,
    recv_a,
    lines_x,
    send_b,
    density,
    spectrum,
    parts,
    tiles,
    pencil,
    pencil_out,
    tiles_in,
    tiles_out,
    plane_in,
    plane,
    slabs,
    arrived,
    cosine,
    sine,
    table_sem,
    load_sem,
    recv_sem,
    recv_b_sem,
    send_sem,
    hart_send,
    hart_recv,
    ) = refs[2 * n_tables + 1 :]
    left_x, left_y, right_z, hart_x, hart_y, hart_z = [tables[i] for i in table_slots]
    g = lax.axis_index("grid")
    o = lax.axis_index("orb")
    layers, _, planes, count_y, count_z = own.shape
    count_x = planes * grid_count
    block_y = count_y // grid_count
    block_k = count_x // orb_count

    def load(l):
        return pltpu.make_async_copy(psi_ref.at[l], own.at[l], load_sem.at[l])

    def fetch(i):
        return pltpu.make_async_copy(tables_hbm[i], tables[i], table_sem.at[i])

    occ_copy = pltpu.make_async_copy(occ_hbm, occ_ref, table_sem.at[n_tables])
    v_copy = pltpu.make_async_copy(v_hbm, v_ref, table_sem.at[n_tables + 1])
    load(0).start()
    for i in range(n_tables):
        fetch(i).start()
    for l in range(1, layers):
        load(l).start()
    occ_copy.start()
    v_copy.start()

    barrier = pltpu.get_barrier_semaphore()

    def greet(axis, me, count):
        def one(off, carry):
            pl.semaphore_signal(
                barrier, inc=1, device_id={axis: lax.rem(me + off, count)}, device_id_type=MESH
            )
            return carry

        lax.fori_loop(1, count, one, 0)

    greet("grid", g, grid_count)
    greet("orb", o, orb_count)

    def send_all(axis, me, count, src, dst, s_sem, r_sem):
        def one(i, carry):
            step = (i + 1) // 2
            to = lax.rem(me + count // 2 + jnp.where(i % 2 == 1, count - step, step), count)
            pltpu.make_async_remote_copy(
                src_ref=src(to),
                dst_ref=dst,
                send_sem=s_sem,
                recv_sem=r_sem,
                device_id={axis: to},
                device_id_type=MESH,
            ).start()
            return carry

        lax.fori_loop(0, count - 1, one, 0)

    def wait_for(ref, sem):
        pltpu.make_async_copy(ref, ref, sem).wait()

    def rows(start, size):
        return pl.ds(pl.multiple_of(start, 8), size)

    def along_y(l):
        load(l).wait()

        def pair(i, carry):
            both = [
                jnp.concatenate([own[l, 0, 2 * i + k], own[l, 1, 2 * i + k]], axis=0) for k in (0, 1)
            ]
            out = dot_table_left(left_y[...], jnp.concatenate(both, axis=1))
            lines_y[2 * i] = out[:, :count_z]
            lines_y[2 * i + 1] = out[:, count_z:]
            return carry

        lax.fori_loop(0, planes // 2, pair, 0)

    half = grid_count // 2
    quarters = [(0, half, half - 1, 1 - half), (half - 2, 2 - half, half - 3, 3 - half), (4, -4, 3, -3), (2, -2, 1, -1)]
    if grid_count != 16:
        quarters = [tuple(range(grid_count))]

    def along_z(l):
        for n, offsets in enumerate(quarters):
            targets = [lax.rem(g + off + grid_count, grid_count) for off in offsets]
            sides = []
            for c in (0, 1):
                blocks = [swap(lines_y[:, rows(c * count_y + to * block_y, block_y), :]) for to in targets]
                sides.append(jnp.concatenate([b.reshape(block_y * planes, count_z) for b in blocks], axis=0))
            out = dot_table_right(jnp.concatenate(sides, axis=1), right_z[...])
            size = block_y * planes
            for k, to in enumerate(targets):
                for c in (0, 1):
                    part = out[k * size : (k + 1) * size, c * count_z : (c + 1) * count_z]
                    send_a[l, pl.ds(to * block_y, block_y), c] = part.reshape(block_y, planes, count_z)
            if l == 0 and n == 0:
                pl.semaphore_wait(barrier, grid_count - 1 + orb_count - 1)
            dst = recv_a.at[l, :, :, rows(g * planes, planes), :]
            for off, to in zip(offsets, targets):
                src = send_a.at[l, pl.ds(to * block_y, block_y)]
                if off == 0:
                    pltpu.make_async_copy(src, dst, recv_sem.at[l]).start()
                else:
                    pltpu.make_async_remote_copy(
                        src_ref=src,
                        dst_ref=dst,
                        send_sem=send_sem.at[0],
                        recv_sem=recv_sem.at[l],
                        device_id={"grid": to},
                        device_id_type=MESH,
                    ).start()

    def forward(l):
        along_y(l)
        along_z(l)

    def sum_modes(y):
        two = dot(hart_x[...], jnp.concatenate([density[y], density[y + 1]], axis=1))
        two = dot(jnp.concatenate([two[:, :count_z], two[:, count_z:]], axis=0), hart_z[...])
        spectrum[y] = two[:count_x]
        spectrum[y + 1] = two[count_x:]
        pair = pl.ds(y, 2)
        send_all(
            "orb",
            o,
            orb_count,
            lambda to: spectrum.at[pair, rows(to * block_k, block_k), :],
            parts.at[o, pair],
            hart_send.at[0],
            hart_recv.at[0],
        )

    def across_x(l):
        wait_for(recv_a.at[l], recv_sem.at[l])
        weight = occ_ref[o * layers + l]

        def pair(i, carry):
            both = [recv_a[l, 2 * i + k].reshape(2 * count_x, count_z) for k in (0, 1)]
            out = dot_table_left(left_x[...], jnp.concatenate(both, axis=1))
            for k in (0, 1):
                part = out[:, k * count_z : (k + 1) * count_z]
                lines_x[2 * i + k] = part
                squares = part[:count_x] * part[:count_x] + part[count_x:] * part[count_x:]
                if l == 0:
                    density[2 * i + k] = weight * squares
                else:
                    density[2 * i + k] += weight * squares
            if l == layers - 1:
                sum_modes(2 * i)
            return carry

        lax.fori_loop(0, block_y // 2, pair, 0)

        def turn(i, carry):
            for c in (0, 1):
                block = lines_x[:, rows(c * count_x + i * planes, planes), :]
                send_b[l, c, rows(i * planes, planes)] = swap(block)
            return carry

        lax.fori_loop(0, grid_count, turn, 0)

    def launch_back(l, c=None):
        part = (slice(None),) if c is None else (c,)

        def src(to):
            return send_b.at[(l, *part, pl.ds(to * planes, planes))]

        dst = arrived.at[(l, *part, slice(None), rows(g * block_y, block_y), slice(None))]
        pltpu.make_async_copy(src(g), dst, recv_b_sem.at[l]).start()
        send_all("grid", g, grid_count, src, dst, send_sem.at[1], recv_b_sem.at[l])

    for i in range(n_tables):
        fetch(i).wait()
    for l in range(layers):
        forward(l)
    occ_copy.wait()
    across_x(0)
    launch_back(0)
    for l in range(1, layers):
        across_x(l)

    wait_for(parts.at[pl.ds(0, orb_count - 1)], hart_recv.at[0])
    own_modes = rows(o * block_k, block_k)
    total = spectrum[:, own_modes, :]
    for off in range(1, orb_count):
        total += parts[lax.rem(o + off, orb_count)]
    tiles[...] = swap(total)

    send_all(
        "grid", g, grid_count, lambda to: tiles.at[to], pencil.at[rows(g * block_y, block_y)], hart_send.at[1], hart_recv.at[1]
    )
    pencil[rows(g * block_y, block_y)] = tiles[g]
    launch_back(1, 0)
    wait_for(pencil.at[pl.ds(0, count_y - block_y)], hart_recv.at[1])

    mode_x = o * block_k + g

    def square(mode, count):
        signed = jnp.where(mode < (count + 1) // 2, mode, mode - count).astype(jnp.float32)
        wave = signed * (2.0 * math.pi / count)
        return wave * wave

    mode_y = lax.broadcasted_iota(jnp.int32, (count_y, count_z), 0)
    mode_z = lax.broadcasted_iota(jnp.int32, (count_y, count_z), 1)
    waves = square(mode_x, count_x) + square(mode_y, count_y) + square(mode_z, count_z)
    anchor = waves <= 0.0
    scale = jnp.where(anchor, 0.0, HARTREE_SCALE / jnp.where(anchor, 1.0, waves))
    pencil_out[...] = dot(hart_y[...], dot(hart_y[...], pencil[...]) * scale)

    send_all(
        "grid", g, grid_count, lambda to: pencil_out.at[rows(to * block_y, block_y)], tiles_in.at[g], hart_send.at[2], hart_recv.at[2]
    )
    tiles_in[g] = pencil_out[rows(g * block_y, block_y)]
    launch_back(1, 1)
    launch_back(2, 0)
    wait_for(tiles_in.at[pl.ds(0, grid_count - 1)], hart_recv.at[2])
    tiles_out[...] = swap(tiles_in[...])

    send_all(
        "orb", o, orb_count, lambda to: tiles_out.at[to], plane_in.at[rows(o * block_k, block_k)], hart_send.at[3], hart_recv.at[3]
    )
    plane_in[rows(o * block_k, block_k)] = tiles_out[o]
    wait_for(plane_in.at[pl.ds(0, count_x - block_k)], hart_recv.at[3])
    plane[...] = dot(dot(hart_x[...], plane_in[...]), hart_z[...])

    mine = slabs.at[o]
    send_all(
        "grid", g, grid_count, lambda to: plane.at[rows(to * planes, planes)], slabs.at[o, g], hart_send.at[4], hart_recv.at[4]
    )
    slabs[o, g] = plane[rows(g * planes, planes)]
    launch_back(2, 1)
    launch_back(3)
    wait_for(mine.at[pl.ds(0, grid_count - 1)], hart_recv.at[4])

    send_all("orb", o, orb_count, lambda to: slabs.at[o], slabs.at[o], hart_send.at[5], hart_recv.at[5])
    wait_for(slabs.at[pl.ds(0, orb_count - 1)], hart_recv.at[5])

    v_copy.wait()

    def spread(i, carry):
        part = rows(i * block_y, block_y)
        theta = TIME_STEP * (v_ref[:, part, :] + swap(slabs[:, i]))
        cosine[:, part, :] = jnp.cos(theta)
        sine[:, part, :] = jnp.sin(theta)
        return carry

    lax.fori_loop(0, grid_count, spread, 0)

    for l in range(layers):
        wait_for(arrived.at[l], recv_b_sem.at[l])

        def turn_phase(x, carry):
            real_part, imag_part = arrived[l, 0, x], arrived[l, 1, x]
            out_ref[l, 0, x] = real_part * cosine[x] + imag_part * sine[x]
            out_ref[l, 1, x] = imag_part * cosine[x] - real_part * sine[x]
            return carry

        lax.fori_loop(0, planes, turn_phase, 0)

    sent_a = send_a.at[:, pl.ds(0, count_y - block_y)]
    wait_for(sent_a, send_sem.at[0])
    sent_b = send_b.at[:, :, pl.ds(0, count_x - planes)]
    wait_for(sent_b, send_sem.at[1])
    wait_for(parts.at[pl.ds(0, orb_count - 1)], hart_send.at[0])
    wait_for(tiles.at[pl.ds(0, grid_count - 1)], hart_send.at[1])
    wait_for(pencil_out.at[pl.ds(0, count_y - block_y)], hart_send.at[2])
    wait_for(tiles_out.at[pl.ds(0, orb_count - 1)], hart_send.at[3])
    wait_for(plane.at[pl.ds(0, count_x - planes)], hart_send.at[4])
    wait_for(slabs.at[pl.ds(0, orb_count - 1)], hart_send.at[5])


def body(grid_count, orb_count, orbitals, v_local, occupations):
    layers, _, planes, count_y, count_z = orbitals.shape
    count_x = planes * grid_count
    block_y = count_y // grid_count
    block_k = count_x // orb_count
    assert block_y == orb_count and block_k == grid_count

    f32 = jnp.float32
    tables = (
        three_parts(kinetic_table(count_x), 1),
        three_parts(kinetic_table(count_y), 1),
        three_parts(kinetic_table(count_z).T, 0),
        hartley_table(count_x),
        hartley_table(count_y),
        hartley_table(count_z),
    )
    keys = [(t.shape, t.tobytes()) for t in tables]
    distinct = list(dict.fromkeys(keys))
    slots = tuple(distinct.index(key) for key in keys)
    tables = [jnp.asarray(tables[keys.index(key)]) for key in distinct]
    anyspace = pl.BlockSpec(memory_space=pltpu.HBM)
    return pl.pallas_call(
        functools.partial(kernel, grid_count, orb_count, slots),
        out_shape=pltpu.VMEM(orbitals.shape, f32),
        in_specs=[anyspace] * (3 + len(tables)),
        out_specs=pl.BlockSpec(memory_space=pltpu.VMEM),
        scratch_shapes=[pltpu.VMEM(t.shape, t.dtype) for t in tables]
        + [
            pltpu.SMEM(occupations.shape, f32),
            pltpu.VMEM(v_local.shape, f32),
            pltpu.VMEM(orbitals.shape, f32),
            pltpu.VMEM((planes, 2 * count_y, count_z), f32),
            pltpu.VMEM((layers, count_y, 2, planes, count_z), f32),
            pltpu.VMEM((layers, block_y, 2, count_x, count_z), f32),
            pltpu.VMEM((block_y, 2 * count_x, count_z), f32),
            pltpu.VMEM((layers, 2, count_x, block_y, count_z), f32),
            pltpu.VMEM((block_y, count_x, count_z), f32),
            pltpu.VMEM((block_y, count_x, count_z), f32),
            pltpu.VMEM((orb_count, block_y, block_k, count_z), f32),
            pltpu.VMEM((grid_count, block_y, count_z), f32),
            pltpu.VMEM((count_y, count_z), f32),
            pltpu.VMEM((count_y, count_z), f32),
            pltpu.VMEM((grid_count, block_y, count_z), f32),
            pltpu.VMEM((block_y, grid_count, count_z), f32),
            pltpu.VMEM((count_x, count_z), f32),
            pltpu.VMEM((count_x, count_z), f32),
            pltpu.VMEM((orb_count, grid_count, planes, count_z), f32),
            pltpu.VMEM(orbitals.shape, f32),
            pltpu.VMEM(v_local.shape, f32),
            pltpu.VMEM(v_local.shape, f32),
            pltpu.SemaphoreType.DMA((len(tables) + 2,)),
            pltpu.SemaphoreType.DMA((layers,)),
            pltpu.SemaphoreType.DMA((layers,)),
            pltpu.SemaphoreType.DMA((layers,)),
            pltpu.SemaphoreType.DMA((2,)),
            pltpu.SemaphoreType.DMA((6,)),
            pltpu.SemaphoreType.DMA((6,)),
        ],
        compiler_params=pltpu.CompilerParams(
            collective_id=0, has_side_effects=True, vmem_limit_bytes=48 * 1024 * 1024
        ),
        name="step",
    )(*[pltpu.with_memory_space_constraint(a, pltpu.HBM) for a in (occupations, orbitals, v_local, *tables)])


def solution(mesh):
    return jax.shard_map(
        functools.partial(body, mesh.shape["grid"], mesh.shape["orb"]),
        mesh=mesh,
        in_specs=(
            P(("groups", "orb"), None, "grid", None, None),
            P(("groups", "grid"), None, None),
            P("groups"),
        ),
        out_specs=P(("groups", "orb"), None, "grid", None, None),
        check_vma=False,
    )
```

```python
import functools
import math

import jax
import jax.numpy as jnp
import numpy as np
from jax import lax
from jax.experimental import pallas as pl
from jax.experimental.pallas import tpu as pltpu
from jax.sharding import PartitionSpec as P

TIME_STEP = 0.05
KINETIC_RATE = 0.1
HARTREE_SCALE = math.pi
HIGHEST = lax.Precision.HIGHEST
MESH = pl.DeviceIdType.MESH


def wave_squared(length):
    mode_ids = np.arange(length)
    signed = np.where(mode_ids < (length + 1) // 2, mode_ids, mode_ids - length)
    return (2.0 * math.pi * signed / length) ** 2


def kinetic_table(length):
    phase = np.exp(-1j * KINETIC_RATE * wave_squared(length))
    circulant = np.fft.ifft(phase)
    ids = np.arange(length)
    full = circulant[(ids[:, None] - ids[None, :]) % length]
    return np.block([[full.real, -full.imag], [full.imag, full.real]]).astype(np.float32)


def hartley_table(length):
    ids = np.arange(length)
    angle = 2.0 * math.pi * (ids[:, None] * ids[None, :] % length) / length
    return ((np.cos(angle) + np.sin(angle)) / math.sqrt(length)).astype(np.float32)


def dot(left, right):
    return jnp.dot(left, right, precision=HIGHEST, preferred_element_type=jnp.float32)


def split(value):
    high = value.astype(jnp.bfloat16)
    return high, (value - high.astype(jnp.float32)).astype(jnp.bfloat16)


def dot_table_left(table, value):
    high, low = split(value)
    stacked = jnp.concatenate([high, high, low], axis=0)
    return jnp.dot(table, stacked, preferred_element_type=jnp.float32)


def dot_table_right(value, table):
    high, low = split(value)
    stacked = jnp.concatenate([high, high, low], axis=1)
    return jnp.dot(stacked, table, preferred_element_type=jnp.float32)


def three_parts(table, axis):
    high = table.astype(jnp.bfloat16)
    low = (table - high.astype(np.float32)).astype(jnp.bfloat16)
    return np.concatenate([high, low, high], axis=axis)


def swap(block):
    return jnp.transpose(block, (1, 0, 2))


def kernel(
    grid_count,
    orb_count,
    table_slots,
    occ_hbm,
    psi_ref,
    v_hbm,
    *refs,
):
    n_tables = len(set(table_slots))
    tables_hbm = refs[:n_tables]
    out_ref = refs[n_tables]
    tables = refs[n_tables + 1 : 2 * n_tables + 1]
    (
    occ_ref,
    v_ref,
    own,
    lines_y,
    send_a,
    recv_a,
    lines_x,
    send_b,
    density,
    spectrum,
    parts,
    tiles,
    pencil,
    pencil_out,
    tiles_in,
    tiles_out,
    plane_in,
    plane,
    slabs,
    arrived,
    cosine,
    sine,
    table_sem,
    load_sem,
    recv_sem,
    recv_b_sem,
    send_sem,
    hart_send,
    hart_recv,
    pair_sem,
    ) = refs[2 * n_tables + 1 :]
    left_x, left_y, right_z, hart_x, hart_y, hart_z = [tables[i] for i in table_slots]
    g = lax.axis_index("grid")
    o = lax.axis_index("orb")
    layers, _, planes, count_y, count_z = own.shape
    count_x = planes * grid_count
    block_y = count_y // grid_count
    block_k = count_x // orb_count

    def load(l):
        return pltpu.make_async_copy(psi_ref.at[l], own.at[l], load_sem.at[l])

    def fetch(i):
        return pltpu.make_async_copy(tables_hbm[i], tables[i], table_sem.at[i])

    occ_copy = pltpu.make_async_copy(occ_hbm, occ_ref, table_sem.at[n_tables])
    v_copy = pltpu.make_async_copy(v_hbm, v_ref, table_sem.at[n_tables + 1])
    load(0).start()
    for i in range(n_tables):
        fetch(i).start()
    for l in range(1, layers):
        load(l).start()
    occ_copy.start()
    v_copy.start()

    barrier = pltpu.get_barrier_semaphore()

    other = g + 1 - 2 * lax.rem(g, 2)

    def greet(axis, me, count, stride):
        def one(k, carry):
            to = lax.rem(me + stride * k, count)
            pl.semaphore_signal(barrier, inc=1, device_id={axis: to}, device_id_type=MESH)
            return carry

        lax.fori_loop(1, count // stride, one, 0)

    greet("grid", g, grid_count, 2)
    pl.semaphore_signal(barrier, inc=1, device_id={"grid": other}, device_id_type=MESH)
    greet("orb", o, orb_count, 1)

    def enter():
        pl.semaphore_wait(barrier, grid_count // 2 + orb_count - 1)
        pl.semaphore_signal(pair_sem, inc=1, device_id={"grid": other}, device_id_type=MESH)

    def send_all(axis, me, count, src, dst, s_sem, r_sem):
        def one(i, carry):
            step = (i + 1) // 2
            to = lax.rem(me + count // 2 + jnp.where(i % 2 == 1, count - step, step), count)
            pltpu.make_async_remote_copy(
                src_ref=src(to),
                dst_ref=dst,
                send_sem=s_sem,
                recv_sem=r_sem,
                device_id={axis: to},
                device_id_type=MESH,
            ).start()
            return carry

        lax.fori_loop(0, count - 1, one, 0)

    def wait_for(ref, sem):
        pltpu.make_async_copy(ref, ref, sem).wait()

    def rows(start, size):
        return pl.ds(pl.multiple_of(start, 8), size)

    def along_y(l):
        load(l).wait()

        def pair(i, carry):
            both = [
                jnp.concatenate([own[l, 0, 2 * i + k], own[l, 1, 2 * i + k]], axis=0) for k in (0, 1)
            ]
            out = dot_table_left(left_y[...], jnp.concatenate(both, axis=1))
            lines_y[2 * i] = out[:, :count_z]
            lines_y[2 * i + 1] = out[:, count_z:]
            return carry

        lax.fori_loop(0, planes // 2, pair, 0)

    half = grid_count // 2
    near = [(4, -4, 3, -3), (2, -2, 1, -1)]
    full = [(0, half, half - 1, 1 - half), (half - 2, 2 - half, half - 3, 3 - half)] + near
    evens = [(half, half - 2, 2 - half, 0), (4, -4, 2, -2)]
    odds = [(half - 1, 1 - half, half - 3, 3 - half), (3, -3, 1, -1)]
    if grid_count != 16:
        full = [tuple(range(grid_count))]
        evens = [tuple(range(0, grid_count, 2))]
        odds = [tuple(range(1, grid_count, 2))]

    def target(off):
        return lax.rem(g + off + grid_count, grid_count)

    def along_z(l, offsets):
        targets = [target(off) for off in offsets]
        sides = []
        for c in (0, 1):
            blocks = [swap(lines_y[:, rows(c * count_y + to * block_y, block_y), :]) for to in targets]
            sides.append(jnp.concatenate([b.reshape(block_y * planes, count_z) for b in blocks], axis=0))
        out = dot_table_right(jnp.concatenate(sides, axis=1), right_z[...])
        size = block_y * planes
        for k, to in enumerate(targets):
            for c in (0, 1):
                part = out[k * size : (k + 1) * size, c * count_z : (c + 1) * count_z]
                send_a[l, pl.ds(to * block_y, block_y), c] = part.reshape(block_y, planes, count_z)

    def launch_forward(l, offsets):
        dst = recv_a.at[l, :, :, rows(g * planes, planes), :]
        for off in offsets:
            to = target(off)
            src = send_a.at[l, pl.ds(to * block_y, block_y)]
            if off == 0:
                pltpu.make_async_copy(src, dst, recv_sem.at[l]).start()
            else:
                pltpu.make_async_remote_copy(
                    src_ref=src,
                    dst_ref=dst,
                    send_sem=send_sem.at[0],
                    recv_sem=recv_sem.at[l],
                    device_id={"grid": to},
                    device_id_type=MESH,
                ).start()

    early = min(2, layers)

    def forward(l):
        along_y(l)
        if l >= early:
            for offsets in full:
                along_z(l, offsets)
                launch_forward(l, offsets)
            return
        for offsets in evens:
            along_z(l, offsets)
            if l == 0 and offsets is evens[0]:
                enter()
            launch_forward(l, offsets)
        for offsets in odds:
            along_z(l, offsets)
        if l == early - 1:
            pl.semaphore_wait(pair_sem, 1)
            for sent in range(early):
                for offsets in odds:
                    launch_forward(sent, offsets)

    def sum_modes(y):
        two = dot(hart_x[...], jnp.concatenate([density[y], density[y + 1]], axis=1))
        two = dot(jnp.concatenate([two[:, :count_z], two[:, count_z:]], axis=0), hart_z[...])
        spectrum[y] = two[:count_x]
        spectrum[y + 1] = two[count_x:]
        pair = pl.ds(y, 2)
        send_all(
            "orb",
            o,
            orb_count,
            lambda to: spectrum.at[pair, rows(to * block_k, block_k), :],
            parts.at[o, pair],
            hart_send.at[0],
            hart_recv.at[0],
        )

    def across_x(l):
        wait_for(recv_a.at[l], recv_sem.at[l])
        weight = occ_ref[o * layers + l]

        def pair(i, carry):
            both = [recv_a[l, 2 * i + k].reshape(2 * count_x, count_z) for k in (0, 1)]
            out = dot_table_left(left_x[...], jnp.concatenate(both, axis=1))
            for k in (0, 1):
                part = out[:, k * count_z : (k + 1) * count_z]
                lines_x[2 * i + k] = part
                squares = part[:count_x] * part[:count_x] + part[count_x:] * part[count_x:]
                if l == 0:
                    density[2 * i + k] = weight * squares
                else:
                    density[2 * i + k] += weight * squares
            if l == layers - 1:
                sum_modes(2 * i)
            return carry

        lax.fori_loop(0, block_y // 2, pair, 0)

        def turn(i, carry):
            for c in (0, 1):
                block = lines_x[:, rows(c * count_x + i * planes, planes), :]
                send_b[l, c, rows(i * planes, planes)] = swap(block)
            return carry

        lax.fori_loop(0, grid_count, turn, 0)

    def launch_back(l, c=None):
        part = (slice(None),) if c is None else (c,)

        def src(to):
            return send_b.at[(l, *part, pl.ds(to * planes, planes))]

        dst = arrived.at[(l, *part, slice(None), rows(g * block_y, block_y), slice(None))]
        pltpu.make_async_copy(src(g), dst, recv_b_sem.at[l]).start()
        send_all("grid", g, grid_count, src, dst, send_sem.at[1], recv_b_sem.at[l])

    for i in range(n_tables):
        fetch(i).wait()
    for l in range(layers):
        forward(l)
    occ_copy.wait()
    across_x(0)
    launch_back(0)
    for l in range(1, layers):
        across_x(l)

    wait_for(parts.at[pl.ds(0, orb_count - 1)], hart_recv.at[0])
    own_modes = rows(o * block_k, block_k)
    total = spectrum[:, own_modes, :]
    for off in range(1, orb_count):
        total += parts[lax.rem(o + off, orb_count)]
    tiles[...] = swap(total)

    send_all(
        "grid", g, grid_count, lambda to: tiles.at[to], pencil.at[rows(g * block_y, block_y)], hart_send.at[1], hart_recv.at[1]
    )
    pencil[rows(g * block_y, block_y)] = tiles[g]
    launch_back(1, 0)
    wait_for(pencil.at[pl.ds(0, count_y - block_y)], hart_recv.at[1])

    mode_x = o * block_k + g

    def square(mode, count):
        signed = jnp.where(mode < (count + 1) // 2, mode, mode - count).astype(jnp.float32)
        wave = signed * (2.0 * math.pi / count)
        return wave * wave

    mode_y = lax.broadcasted_iota(jnp.int32, (count_y, count_z), 0)
    mode_z = lax.broadcasted_iota(jnp.int32, (count_y, count_z), 1)
    waves = square(mode_x, count_x) + square(mode_y, count_y) + square(mode_z, count_z)
    anchor = waves <= 0.0
    scale = jnp.where(anchor, 0.0, HARTREE_SCALE / jnp.where(anchor, 1.0, waves))
    pencil_out[...] = dot(hart_y[...], dot(hart_y[...], pencil[...]) * scale)

    send_all(
        "grid", g, grid_count, lambda to: pencil_out.at[rows(to * block_y, block_y)], tiles_in.at[g], hart_send.at[2], hart_recv.at[2]
    )
    tiles_in[g] = pencil_out[rows(g * block_y, block_y)]
    launch_back(1, 1)
    launch_back(2, 0)
    wait_for(tiles_in.at[pl.ds(0, grid_count - 1)], hart_recv.at[2])
    tiles_out[...] = swap(tiles_in[...])

    send_all(
        "orb", o, orb_count, lambda to: tiles_out.at[to], plane_in.at[rows(o * block_k, block_k)], hart_send.at[3], hart_recv.at[3]
    )
    plane_in[rows(o * block_k, block_k)] = tiles_out[o]
    wait_for(plane_in.at[pl.ds(0, count_x - block_k)], hart_recv.at[3])
    plane[...] = dot(dot(hart_x[...], plane_in[...]), hart_z[...])

    mine = slabs.at[o]
    send_all(
        "grid", g, grid_count, lambda to: plane.at[rows(to * planes, planes)], slabs.at[o, g], hart_send.at[4], hart_recv.at[4]
    )
    slabs[o, g] = plane[rows(g * planes, planes)]
    launch_back(2, 1)
    launch_back(3)
    wait_for(mine.at[pl.ds(0, grid_count - 1)], hart_recv.at[4])

    send_all("orb", o, orb_count, lambda to: slabs.at[o], slabs.at[o], hart_send.at[5], hart_recv.at[5])
    wait_for(slabs.at[pl.ds(0, orb_count - 1)], hart_recv.at[5])

    v_copy.wait()

    def spread(i, carry):
        part = rows(i * block_y, block_y)
        theta = TIME_STEP * (v_ref[:, part, :] + swap(slabs[:, i]))
        cosine[:, part, :] = jnp.cos(theta)
        sine[:, part, :] = jnp.sin(theta)
        return carry

    lax.fori_loop(0, grid_count, spread, 0)

    for l in range(layers):
        wait_for(arrived.at[l], recv_b_sem.at[l])

        def turn_phase(x, carry):
            real_part, imag_part = arrived[l, 0, x], arrived[l, 1, x]
            out_ref[l, 0, x] = real_part * cosine[x] + imag_part * sine[x]
            out_ref[l, 1, x] = imag_part * cosine[x] - real_part * sine[x]
            return carry

        lax.fori_loop(0, planes, turn_phase, 0)

    sent_a = send_a.at[:, pl.ds(0, count_y - block_y)]
    wait_for(sent_a, send_sem.at[0])
    sent_b = send_b.at[:, :, pl.ds(0, count_x - planes)]
    wait_for(sent_b, send_sem.at[1])
    wait_for(parts.at[pl.ds(0, orb_count - 1)], hart_send.at[0])
    wait_for(tiles.at[pl.ds(0, grid_count - 1)], hart_send.at[1])
    wait_for(pencil_out.at[pl.ds(0, count_y - block_y)], hart_send.at[2])
    wait_for(tiles_out.at[pl.ds(0, orb_count - 1)], hart_send.at[3])
    wait_for(plane.at[pl.ds(0, count_x - planes)], hart_send.at[4])
    wait_for(slabs.at[pl.ds(0, orb_count - 1)], hart_send.at[5])


def body(grid_count, orb_count, orbitals, v_local, occupations):
    layers, _, planes, count_y, count_z = orbitals.shape
    count_x = planes * grid_count
    block_y = count_y // grid_count
    block_k = count_x // orb_count
    assert block_y == orb_count and block_k == grid_count

    f32 = jnp.float32
    tables = (
        three_parts(kinetic_table(count_x), 1),
        three_parts(kinetic_table(count_y), 1),
        three_parts(kinetic_table(count_z).T, 0),
        hartley_table(count_x),
        hartley_table(count_y),
        hartley_table(count_z),
    )
    keys = [(t.shape, t.tobytes()) for t in tables]
    distinct = list(dict.fromkeys(keys))
    slots = tuple(distinct.index(key) for key in keys)
    tables = [jnp.asarray(tables[keys.index(key)]) for key in distinct]
    anyspace = pl.BlockSpec(memory_space=pltpu.HBM)
    return pl.pallas_call(
        functools.partial(kernel, grid_count, orb_count, slots),
        out_shape=pltpu.VMEM(orbitals.shape, f32),
        in_specs=[anyspace] * (3 + len(tables)),
        out_specs=pl.BlockSpec(memory_space=pltpu.VMEM),
        scratch_shapes=[pltpu.VMEM(t.shape, t.dtype) for t in tables]
        + [
            pltpu.SMEM(occupations.shape, f32),
            pltpu.VMEM(v_local.shape, f32),
            pltpu.VMEM(orbitals.shape, f32),
            pltpu.VMEM((planes, 2 * count_y, count_z), f32),
            pltpu.VMEM((layers, count_y, 2, planes, count_z), f32),
            pltpu.VMEM((layers, block_y, 2, count_x, count_z), f32),
            pltpu.VMEM((block_y, 2 * count_x, count_z), f32),
            pltpu.VMEM((layers, 2, count_x, block_y, count_z), f32),
            pltpu.VMEM((block_y, count_x, count_z), f32),
            pltpu.VMEM((block_y, count_x, count_z), f32),
            pltpu.VMEM((orb_count, block_y, block_k, count_z), f32),
            pltpu.VMEM((grid_count, block_y, count_z), f32),
            pltpu.VMEM((count_y, count_z), f32),
            pltpu.VMEM((count_y, count_z), f32),
            pltpu.VMEM((grid_count, block_y, count_z), f32),
            pltpu.VMEM((block_y, grid_count, count_z), f32),
            pltpu.VMEM((count_x, count_z), f32),
            pltpu.VMEM((count_x, count_z), f32),
            pltpu.VMEM((orb_count, grid_count, planes, count_z), f32),
            pltpu.VMEM(orbitals.shape, f32),
            pltpu.VMEM(v_local.shape, f32),
            pltpu.VMEM(v_local.shape, f32),
            pltpu.SemaphoreType.DMA((len(tables) + 2,)),
            pltpu.SemaphoreType.DMA((layers,)),
            pltpu.SemaphoreType.DMA((layers,)),
            pltpu.SemaphoreType.DMA((layers,)),
            pltpu.SemaphoreType.DMA((2,)),
            pltpu.SemaphoreType.DMA((6,)),
            pltpu.SemaphoreType.DMA((6,)),
            pltpu.SemaphoreType.REGULAR,
        ],
        compiler_params=pltpu.CompilerParams(
            collective_id=0, has_side_effects=True, vmem_limit_bytes=48 * 1024 * 1024
        ),
        name="step",
    )(*[pltpu.with_memory_space_constraint(a, pltpu.HBM) for a in (occupations, orbitals, v_local, *tables)])


def solution(mesh):
    return jax.shard_map(
        functools.partial(body, mesh.shape["grid"], mesh.shape["orb"]),
        mesh=mesh,
        in_specs=(
            P(("groups", "orb"), None, "grid", None, None),
            P(("groups", "grid"), None, None),
            P("groups"),
        ),
        out_specs=P(("groups", "orb"), None, "grid", None, None),
        check_vma=False,
    )
```

```python
import functools
import math

import jax
import jax.numpy as jnp
import numpy as np
from jax import lax
from jax.experimental import pallas as pl
from jax.experimental.pallas import tpu as pltpu
from jax.sharding import PartitionSpec as P

TIME_STEP = 0.05
KINETIC_RATE = 0.1
HARTREE_SCALE = math.pi
HIGHEST = lax.Precision.HIGHEST
MESH = pl.DeviceIdType.MESH


def wave_squared(length):
    mode_ids = np.arange(length)
    signed = np.where(mode_ids < (length + 1) // 2, mode_ids, mode_ids - length)
    return (2.0 * math.pi * signed / length) ** 2


def kinetic_table(length):
    phase = np.exp(-1j * KINETIC_RATE * wave_squared(length))
    circulant = np.fft.ifft(phase)
    ids = np.arange(length)
    full = circulant[(ids[:, None] - ids[None, :]) % length]
    return np.block([[full.real, -full.imag], [full.imag, full.real]]).astype(np.float32)


def hartley_table(length):
    ids = np.arange(length)
    angle = 2.0 * math.pi * (ids[:, None] * ids[None, :] % length) / length
    return ((np.cos(angle) + np.sin(angle)) / math.sqrt(length)).astype(np.float32)


def dot(left, right):
    return jnp.dot(left, right, precision=HIGHEST, preferred_element_type=jnp.float32)


def split(value):
    high = value.astype(jnp.bfloat16)
    return high, (value - high.astype(jnp.float32)).astype(jnp.bfloat16)


def dot_table_left(table, value):
    high, low = split(value)
    stacked = jnp.concatenate([high, high, low], axis=0)
    return jnp.dot(table, stacked, preferred_element_type=jnp.float32)


def dot_table_right(value, table):
    high, low = split(value)
    stacked = jnp.concatenate([high, high, low], axis=1)
    return jnp.dot(stacked, table, preferred_element_type=jnp.float32)


def three_parts(table, axis):
    high = table.astype(jnp.bfloat16)
    low = (table - high.astype(np.float32)).astype(jnp.bfloat16)
    return np.concatenate([high, low, high], axis=axis)


def swap(block):
    return jnp.transpose(block, (1, 0, 2))


def kernel(
    grid_count,
    orb_count,
    table_slots,
    occ_hbm,
    psi_ref,
    v_hbm,
    *refs,
):
    n_tables = len(set(table_slots))
    tables_hbm = refs[:n_tables]
    out_ref = refs[n_tables]
    tables = refs[n_tables + 1 : 2 * n_tables + 1]
    (
    occ_ref,
    v_ref,
    own,
    lines_y,
    send_a,
    recv_a,
    lines_x,
    send_b,
    density,
    spectrum,
    parts,
    tiles,
    pencil,
    pencil_out,
    tiles_in,
    tiles_out,
    plane_in,
    plane,
    slabs,
    arrived,
    cosine,
    sine,
    table_sem,
    load_sem,
    recv_sem,
    recv_b_sem,
    send_sem,
    hart_send,
    hart_recv,
    pair_sem,
    ) = refs[2 * n_tables + 1 :]
    left_x, left_y, right_z, hart_x, hart_y, hart_z = [tables[i] for i in table_slots]
    g = lax.axis_index("grid")
    o = lax.axis_index("orb")
    layers, _, planes, count_y, count_z = own.shape
    count_x = planes * grid_count
    block_y = count_y // grid_count
    block_k = count_x // orb_count

    def load(l):
        return pltpu.make_async_copy(psi_ref.at[l], own.at[l], load_sem.at[l])

    def fetch(i):
        return pltpu.make_async_copy(tables_hbm[i], tables[i], table_sem.at[i])

    occ_copy = pltpu.make_async_copy(occ_hbm, occ_ref, table_sem.at[n_tables])
    v_copy = pltpu.make_async_copy(v_hbm, v_ref, table_sem.at[n_tables + 1])
    load(0).start()
    for i in range(n_tables):
        fetch(i).start()
    for l in range(1, layers):
        load(l).start()
    occ_copy.start()
    v_copy.start()

    barrier = pltpu.get_barrier_semaphore()

    other = g + 1 - 2 * lax.rem(g, 2)

    def greet(axis, me, count, stride):
        def one(k, carry):
            to = lax.rem(me + stride * k, count)
            pl.semaphore_signal(barrier, inc=1, device_id={axis: to}, device_id_type=MESH)
            return carry

        lax.fori_loop(1, count // stride, one, 0)

    greet("grid", g, grid_count, 2)
    pl.semaphore_signal(barrier, inc=1, device_id={"grid": other}, device_id_type=MESH)
    greet("orb", o, orb_count, 1)

    def enter():
        pl.semaphore_wait(barrier, grid_count // 2 + orb_count - 1)
        pl.semaphore_signal(pair_sem, inc=1, device_id={"grid": other}, device_id_type=MESH)

    def send_all(axis, me, count, src, dst, s_sem, r_sem):
        def one(i, carry):
            step = (i + 1) // 2
            to = lax.rem(me + count // 2 + jnp.where(i % 2 == 1, count - step, step), count)
            pltpu.make_async_remote_copy(
                src_ref=src(to),
                dst_ref=dst,
                send_sem=s_sem,
                recv_sem=r_sem,
                device_id={axis: to},
                device_id_type=MESH,
            ).start()
            return carry

        lax.fori_loop(0, count - 1, one, 0)

    def wait_for(ref, sem):
        pltpu.make_async_copy(ref, ref, sem).wait()

    def rows(start, size):
        return pl.ds(pl.multiple_of(start, 8), size)

    def along_y(l):
        load(l).wait()

        def pair(i, carry):
            both = [
                jnp.concatenate([own[l, 0, 2 * i + k], own[l, 1, 2 * i + k]], axis=0) for k in (0, 1)
            ]
            out = dot_table_left(left_y[...], jnp.concatenate(both, axis=1))
            lines_y[2 * i] = out[:, :count_z]
            lines_y[2 * i + 1] = out[:, count_z:]
            return carry

        lax.fori_loop(0, planes // 2, pair, 0)

    half = grid_count // 2
    near = [(4, -4, 3, -3), (2, -2, 1, -1)]
    full = [(0, half, half - 1, 1 - half), (half - 2, 2 - half, half - 3, 3 - half)] + near
    evens = [(half, half - 2, 2 - half, 0), (4, -4, 2, -2)]
    odds = [(half - 1, 1 - half, half - 3, 3 - half), (3, -3, 1, -1)]
    if grid_count != 16:
        full = [tuple(range(grid_count))]
        evens = [tuple(range(0, grid_count, 2))]
        odds = [tuple(range(1, grid_count, 2))]

    def target(off):
        return lax.rem(g + off + grid_count, grid_count)

    def along_z(l, offsets):
        targets = [target(off) for off in offsets]
        sides = []
        for c in (0, 1):
            blocks = [swap(lines_y[:, rows(c * count_y + to * block_y, block_y), :]) for to in targets]
            sides.append(jnp.concatenate([b.reshape(block_y * planes, count_z) for b in blocks], axis=0))
        out = dot_table_right(jnp.concatenate(sides, axis=1), right_z[...])
        size = block_y * planes
        for k, to in enumerate(targets):
            for c in (0, 1):
                part = out[k * size : (k + 1) * size, c * count_z : (c + 1) * count_z]
                send_a[l, pl.ds(to * block_y, block_y), c] = part.reshape(block_y, planes, count_z)

    def launch_forward(l, offsets):
        dst = recv_a.at[l, :, :, rows(g * planes, planes), :]
        for off in offsets:
            to = target(off)
            src = send_a.at[l, pl.ds(to * block_y, block_y)]
            if off == 0:
                pltpu.make_async_copy(src, dst, recv_sem.at[l]).start()
            else:
                pltpu.make_async_remote_copy(
                    src_ref=src,
                    dst_ref=dst,
                    send_sem=send_sem.at[0],
                    recv_sem=recv_sem.at[l],
                    device_id={"grid": to},
                    device_id_type=MESH,
                ).start()

    early = min(3, layers)

    def forward(l):
        along_y(l)
        if l >= early:
            for offsets in full:
                along_z(l, offsets)
                launch_forward(l, offsets)
            return
        for offsets in evens:
            along_z(l, offsets)
            if l == 0 and offsets is evens[0]:
                enter()
            launch_forward(l, offsets)
        for offsets in odds:
            along_z(l, offsets)
        if l == early - 1:
            pl.semaphore_wait(pair_sem, 1)
            for sent in range(early):
                for offsets in odds:
                    launch_forward(sent, offsets)

    def sum_modes(y):
        two = dot(hart_x[...], jnp.concatenate([density[y], density[y + 1]], axis=1))
        two = dot(jnp.concatenate([two[:, :count_z], two[:, count_z:]], axis=0), hart_z[...])
        spectrum[y] = two[:count_x]
        spectrum[y + 1] = two[count_x:]
        pair = pl.ds(y, 2)
        send_all(
            "orb",
            o,
            orb_count,
            lambda to: spectrum.at[pair, rows(to * block_k, block_k), :],
            parts.at[o, pair],
            hart_send.at[0],
            hart_recv.at[0],
        )

    def across_x(l):
        wait_for(recv_a.at[l], recv_sem.at[l])
        weight = occ_ref[o * layers + l]

        def pair(i, carry):
            both = [recv_a[l, 2 * i + k].reshape(2 * count_x, count_z) for k in (0, 1)]
            out = dot_table_left(left_x[...], jnp.concatenate(both, axis=1))
            for k in (0, 1):
                part = out[:, k * count_z : (k + 1) * count_z]
                lines_x[2 * i + k] = part
                squares = part[:count_x] * part[:count_x] + part[count_x:] * part[count_x:]
                if l == 0:
                    density[2 * i + k] = weight * squares
                else:
                    density[2 * i + k] += weight * squares
            if l == layers - 1:
                sum_modes(2 * i)
            return carry

        lax.fori_loop(0, block_y // 2, pair, 0)

        def turn(i, carry):
            for c in (0, 1):
                block = lines_x[:, rows(c * count_x + i * planes, planes), :]
                send_b[l, c, rows(i * planes, planes)] = swap(block)
            return carry

        lax.fori_loop(0, grid_count, turn, 0)

    def launch_back(l, c=None):
        part = (slice(None),) if c is None else (c,)

        def src(to):
            return send_b.at[(l, *part, pl.ds(to * planes, planes))]

        dst = arrived.at[(l, *part, slice(None), rows(g * block_y, block_y), slice(None))]
        pltpu.make_async_copy(src(g), dst, recv_b_sem.at[l]).start()
        send_all("grid", g, grid_count, src, dst, send_sem.at[1], recv_b_sem.at[l])

    for i in range(n_tables):
        fetch(i).wait()
    for l in range(layers):
        forward(l)
    occ_copy.wait()
    across_x(0)
    launch_back(0)
    for l in range(1, layers):
        across_x(l)

    wait_for(parts.at[pl.ds(0, orb_count - 1)], hart_recv.at[0])
    own_modes = rows(o * block_k, block_k)
    total = spectrum[:, own_modes, :]
    for off in range(1, orb_count):
        total += parts[lax.rem(o + off, orb_count)]
    tiles[...] = swap(total)

    send_all(
        "grid", g, grid_count, lambda to: tiles.at[to], pencil.at[rows(g * block_y, block_y)], hart_send.at[1], hart_recv.at[1]
    )
    pencil[rows(g * block_y, block_y)] = tiles[g]
    launch_back(1, 0)
    wait_for(pencil.at[pl.ds(0, count_y - block_y)], hart_recv.at[1])

    mode_x = o * block_k + g

    def square(mode, count):
        signed = jnp.where(mode < (count + 1) // 2, mode, mode - count).astype(jnp.float32)
        wave = signed * (2.0 * math.pi / count)
        return wave * wave

    mode_y = lax.broadcasted_iota(jnp.int32, (count_y, count_z), 0)
    mode_z = lax.broadcasted_iota(jnp.int32, (count_y, count_z), 1)
    waves = square(mode_x, count_x) + square(mode_y, count_y) + square(mode_z, count_z)
    anchor = waves <= 0.0
    scale = jnp.where(anchor, 0.0, HARTREE_SCALE / jnp.where(anchor, 1.0, waves))
    pencil_out[...] = dot(hart_y[...], dot(hart_y[...], pencil[...]) * scale)

    send_all(
        "grid", g, grid_count, lambda to: pencil_out.at[rows(to * block_y, block_y)], tiles_in.at[g], hart_send.at[2], hart_recv.at[2]
    )
    tiles_in[g] = pencil_out[rows(g * block_y, block_y)]
    launch_back(1, 1)
    launch_back(2, 0)
    wait_for(tiles_in.at[pl.ds(0, grid_count - 1)], hart_recv.at[2])
    tiles_out[...] = swap(tiles_in[...])

    send_all(
        "orb", o, orb_count, lambda to: tiles_out.at[to], plane_in.at[rows(o * block_k, block_k)], hart_send.at[3], hart_recv.at[3]
    )
    plane_in[rows(o * block_k, block_k)] = tiles_out[o]
    wait_for(plane_in.at[pl.ds(0, count_x - block_k)], hart_recv.at[3])
    plane[...] = dot(dot(hart_x[...], plane_in[...]), hart_z[...])

    mine = slabs.at[o]
    send_all(
        "grid", g, grid_count, lambda to: plane.at[rows(to * planes, planes)], slabs.at[o, g], hart_send.at[4], hart_recv.at[4]
    )
    slabs[o, g] = plane[rows(g * planes, planes)]
    launch_back(2, 1)
    launch_back(3)
    wait_for(mine.at[pl.ds(0, grid_count - 1)], hart_recv.at[4])

    send_all("orb", o, orb_count, lambda to: slabs.at[o], slabs.at[o], hart_send.at[5], hart_recv.at[5])
    wait_for(slabs.at[pl.ds(0, orb_count - 1)], hart_recv.at[5])

    v_copy.wait()

    def spread(i, carry):
        part = rows(i * block_y, block_y)
        theta = TIME_STEP * (v_ref[:, part, :] + swap(slabs[:, i]))
        cosine[:, part, :] = jnp.cos(theta)
        sine[:, part, :] = jnp.sin(theta)
        return carry

    lax.fori_loop(0, grid_count, spread, 0)

    for l in range(layers):
        wait_for(arrived.at[l], recv_b_sem.at[l])

        def turn_phase(x, carry):
            real_part, imag_part = arrived[l, 0, x], arrived[l, 1, x]
            out_ref[l, 0, x] = real_part * cosine[x] + imag_part * sine[x]
            out_ref[l, 1, x] = imag_part * cosine[x] - real_part * sine[x]
            return carry

        lax.fori_loop(0, planes, turn_phase, 0)

    sent_a = send_a.at[:, pl.ds(0, count_y - block_y)]
    wait_for(sent_a, send_sem.at[0])
    sent_b = send_b.at[:, :, pl.ds(0, count_x - planes)]
    wait_for(sent_b, send_sem.at[1])
    wait_for(parts.at[pl.ds(0, orb_count - 1)], hart_send.at[0])
    wait_for(tiles.at[pl.ds(0, grid_count - 1)], hart_send.at[1])
    wait_for(pencil_out.at[pl.ds(0, count_y - block_y)], hart_send.at[2])
    wait_for(tiles_out.at[pl.ds(0, orb_count - 1)], hart_send.at[3])
    wait_for(plane.at[pl.ds(0, count_x - planes)], hart_send.at[4])
    wait_for(slabs.at[pl.ds(0, orb_count - 1)], hart_send.at[5])


def body(grid_count, orb_count, orbitals, v_local, occupations):
    layers, _, planes, count_y, count_z = orbitals.shape
    count_x = planes * grid_count
    block_y = count_y // grid_count
    block_k = count_x // orb_count
    assert block_y == orb_count and block_k == grid_count

    f32 = jnp.float32
    tables = (
        three_parts(kinetic_table(count_x), 1),
        three_parts(kinetic_table(count_y), 1),
        three_parts(kinetic_table(count_z).T, 0),
        hartley_table(count_x),
        hartley_table(count_y),
        hartley_table(count_z),
    )
    keys = [(t.shape, t.tobytes()) for t in tables]
    distinct = list(dict.fromkeys(keys))
    slots = tuple(distinct.index(key) for key in keys)
    tables = [jnp.asarray(tables[keys.index(key)]) for key in distinct]
    anyspace = pl.BlockSpec(memory_space=pltpu.HBM)
    return pl.pallas_call(
        functools.partial(kernel, grid_count, orb_count, slots),
        out_shape=pltpu.VMEM(orbitals.shape, f32),
        in_specs=[anyspace] * (3 + len(tables)),
        out_specs=pl.BlockSpec(memory_space=pltpu.VMEM),
        scratch_shapes=[pltpu.VMEM(t.shape, t.dtype) for t in tables]
        + [
            pltpu.SMEM(occupations.shape, f32),
            pltpu.VMEM(v_local.shape, f32),
            pltpu.VMEM(orbitals.shape, f32),
            pltpu.VMEM((planes, 2 * count_y, count_z), f32),
            pltpu.VMEM((layers, count_y, 2, planes, count_z), f32),
            pltpu.VMEM((layers, block_y, 2, count_x, count_z), f32),
            pltpu.VMEM((block_y, 2 * count_x, count_z), f32),
            pltpu.VMEM((layers, 2, count_x, block_y, count_z), f32),
            pltpu.VMEM((block_y, count_x, count_z), f32),
            pltpu.VMEM((block_y, count_x, count_z), f32),
            pltpu.VMEM((orb_count, block_y, block_k, count_z), f32),
            pltpu.VMEM((grid_count, block_y, count_z), f32),
            pltpu.VMEM((count_y, count_z), f32),
            pltpu.VMEM((count_y, count_z), f32),
            pltpu.VMEM((grid_count, block_y, count_z), f32),
            pltpu.VMEM((block_y, grid_count, count_z), f32),
            pltpu.VMEM((count_x, count_z), f32),
            pltpu.VMEM((count_x, count_z), f32),
            pltpu.VMEM((orb_count, grid_count, planes, count_z), f32),
            pltpu.VMEM(orbitals.shape, f32),
            pltpu.VMEM(v_local.shape, f32),
            pltpu.VMEM(v_local.shape, f32),
            pltpu.SemaphoreType.DMA((len(tables) + 2,)),
            pltpu.SemaphoreType.DMA((layers,)),
            pltpu.SemaphoreType.DMA((layers,)),
            pltpu.SemaphoreType.DMA((layers,)),
            pltpu.SemaphoreType.DMA((2,)),
            pltpu.SemaphoreType.DMA((6,)),
            pltpu.SemaphoreType.DMA((6,)),
            pltpu.SemaphoreType.REGULAR,
        ],
        compiler_params=pltpu.CompilerParams(
            collective_id=0, has_side_effects=True, vmem_limit_bytes=48 * 1024 * 1024
        ),
        name="step",
    )(*[pltpu.with_memory_space_constraint(a, pltpu.HBM) for a in (occupations, orbitals, v_local, *tables)])


def solution(mesh):
    return jax.shard_map(
        functools.partial(body, mesh.shape["grid"], mesh.shape["orb"]),
        mesh=mesh,
        in_specs=(
            P(("groups", "orb"), None, "grid", None, None),
            P(("groups", "grid"), None, None),
            P("groups"),
        ),
        out_specs=P(("groups", "orb"), None, "grid", None, None),
        check_vma=False,
    )
```
